128 devices in a mesh: gx: 4 (over x), gy: 8 (over z, y_lo), gz: 4 (over y_hi, core).
Axes of the slice: x: 4, y: 4 (y_hi: 2, y_lo: 2; y = y_hi * 2 + y_lo), z: 4, core: 2. Of those that a mesh axis runs over, the one named last changes fastest.
Arguments:
- tokens: bfloat16 [4096, 6144], P('gy', ('gz', 'gx')), may hold values from -6 to 6
- weight: bfloat16 [6144, 24576], P('gz', ('gx', 'gy')), may hold values from -0.15625 to 0.15625
- bias: float32 [24576], P(('gx', 'gz')), may hold values from -4 to 4
Outputs:
- hidden: bfloat16 [4096, 24576], P('gy', ('gx', 'gz'))
The draws below stay inside these ranges and needn't reach their ends.
All inputs are finite; a program needn't handle non-finite values.
Results may differ from the reference program's by a relative error of at most 0.001.
Values may be sent and summed in bfloat16 or wider, within the bound.
A program may use at most 128 MiB of HBM per device.

```python
import jax
import jax.numpy as jnp

D = 6144
FF = 24576
TOKENS = 4096


def spiked(values, rng, source, target, shards_of, factor):
    owner, partner = [(jnp.arange(values.shape[axis_at]) // (values.shape[axis_at] // shards_of)).reshape([-1 if axis == axis_at else 1 for axis in range(values.ndim)]) for axis_at in (source, target)]
    chosen = jax.random.permutation(rng, shards_of)[partner]
    strong = (owner == chosen) | (owner == (partner + shards_of // 2) % shards_of)
    return jnp.where(strong, factor * values, values)


def level_of(key, dims, split, least, high):
    level = 1.0
    for position, shards_of in split:
        heights = jax.random.uniform(jax.random.fold_in(jax.random.fold_in(key, 6), position), (shards_of,), jnp.float32, least / len(split), high / len(split))
        level = level * jnp.repeat(jnp.exp(heights), dims[position] // shards_of).reshape((-1,) + (1,) * (len(dims) - 1 - position))
    return level


def scatter_about(key, extent, width, limit, shards=(), held_as=jnp.bfloat16):
    drawn = width * jax.random.normal(key, extent, jnp.float32)
    if shards:
        drawn = drawn * level_of(key, extent, shards, -0.22, 0.18)
    return jnp.clip(drawn, -limit, limit).astype(held_as)


def heavy_noise(stream_key, shape, spread, limit, cuts, heavy, kind=jnp.bfloat16):
    array = spread * jax.random.normal(stream_key, shape, jnp.float32)
    if cuts:
        array = array * level_of(stream_key, shape, cuts, -0.22, 0.18)
    return jnp.clip(spiked(array, jax.random.fold_in(stream_key, 3), *heavy), -limit, limit).astype(kind)


def setup_inputs(seed: int = 0) -> dict:
    key_list = jax.random.split(jax.random.key(seed), 4)
    return {
        "tokens": scatter_about(key_list[0], (TOKENS, D), 1.0, 6.0, ((0, 8), (1, 16))),
        "weight": heavy_noise(key_list[1], (D, FF), D ** -0.5, 0.15625, ((0, 4), (1, 32)), (0, 1, 32, 2.75)),
        "bias": scatter_about(key_list[2], (FF,), 1.0, 4.0, ((0, 16),), jnp.float32),
    }


def reference(tokens, weight, bias):
    pre = jnp.dot(tokens, weight, preferred_element_type=jnp.float32) + bias.astype(jnp.float32)
    return jax.nn.gelu(pre, approximate=False).astype(jnp.bfloat16)
```

```python
import jax
import jax.numpy as jnp
from jax import lax
from jax.experimental import pallas as pl
from jax.experimental.pallas import tpu as pltpu
from jax.sharding import Mesh
from jax.sharding import PartitionSpec as P

MESH = pl.DeviceIdType.MESH
S = 384
ROWS = 512
D = 6144
TILE = 256


def kernel(
    t_ref, w_ref, b_ref, o_ref,
    T, W, B, O,
    tsem, wsem, bsem, osem,
    ts_y, ts_x, ts_r, ws_a, ws_b, ws_n, ws_r, ws_f, bs, os,
):
    x, z, l, h, c = (lax.axis_index(a) for a in ("x", "z", "l", "h", "c"))
    y = 2 * h + l
    g = 2 * h + c
    other = 1 - c
    xp, xm, xf = (x + 1) % 4, (x + 3) % 4, (x + 2) % 4
    zp, zm, zf = (z + 1) % 4, (z + 3) % 4, (z + 2) % 4
    yp, ym = (y + 1) % 4, (y + 3) % 4
    order = [2 * hh + cc for hh in (h, 1 - h) for cc in (0, 1)]
    kinds = [g, 2 * (1 - h) + c]
    sibling = {"c": other}
    sends = []

    def token(gg, xx):
        return T.at[:, pl.ds(pl.multiple_of((gg * 4 + xx) * S, S), S)]

    def weight(zz, gg, i):
        return W.at[zz, pl.ds(pl.multiple_of(gg * 4 * S + i * S, S), S), :]

    def shard(i, half):
        return w_ref.at[pl.ds(i * S, S), pl.ds(pl.multiple_of(half * S, S), S)]

    def push(src, dst, send, recv, to):
        copy = pltpu.make_async_remote_copy(
            src_ref=src, dst_ref=dst, send_sem=send, recv_sem=recv,
            device_id=to, device_id_type=MESH,
        )
        copy.start()
        sends.append(copy)

    def landed(slot, sem):
        pltpu.make_async_copy(slot, slot, sem).wait()

    def push_token(gg, xx, send, to):
        push(token(gg, xx), token(gg, xx), send, tsem.at[gg, xx], to)

    def push_weight(zz, gg, i, send, to):
        push(weight(zz, gg, i), weight(zz, gg, i), send, wsem.at[zz, gg, i], to)

    @pl.when(c == l)
    def _():
        pltpu.make_async_copy(t_ref, token(g, x), tsem.at[g, x]).start()

    for i in range(4):
        pltpu.make_async_copy(shard(i, h), weight(z, g, i), wsem.at[z, g, i]).start()
    pltpu.make_async_copy(b_ref, B.at[0], bsem.at[0]).start()

    barrier = pltpu.get_barrier_semaphore()
    peers = [
        {"l": (l + dl) % 2, "h": (h + dh) % 2, "c": (c + dc) % 2}
        for dl in (0, 1) for dh in (0, 1) for dc in (0, 1) if dl + dh + dc
    ]
    peers += [{"x": xp}, {"x": xm}, {"z": zp}, {"z": zm}]
    for peer in peers:
        pl.semaphore_signal(barrier, inc=1, device_id=peer, device_id_type=MESH)
    pl.semaphore_wait(barrier, len(peers))

    def to_own_chip():
        return pltpu.make_async_remote_copy(
            src_ref=t_ref, dst_ref=token(g, x), send_sem=ts_y.at[3], recv_sem=tsem.at[g, x],
            device_id=sibling, device_id_type=MESH,
        )

    @pl.when(c != l)
    def _():
        to_own_chip().start()

    for k, yy in enumerate((yp, ym, (y + 2) % 4)):
        push(t_ref, token(g, x), ts_y.at[k], tsem.at[g, x], {"l": yy % 2, "h": yy // 2, "c": l})
    for i in range(4):
        push(shard(i, h), weight(z, g, i), ws_a.at[i, 0], wsem.at[z, g, i], {"z": zp})
        push(shard(i, h), weight(z, g, i), ws_a.at[i, 1], wsem.at[z, g, i], {"z": zm})
        push(shard(i, 1 - h), weight(z, g, i), ws_a.at[i, 3], wsem.at[z, g, i], {"h": 1 - h})
        push(shard(i, h), weight(z, g, i), ws_a.at[i, 2], wsem.at[z, g, i], sibling)
    for k, (dh, dc) in enumerate(((0, 1), (1, 0), (1, 1))):
        to = {"h": (h + dh) % 2, "c": (c + dc) % 2}
        push(b_ref, B.at[1 + k], bs.at[k], bsem.at[1 + k], to)

    def token_y(q):
        gg = order[q]
        landed(token(gg, x), tsem.at[gg, x])
        push_token(gg, x, ts_x.at[q, 0], {"x": xp})
        push_token(gg, x, ts_x.at[q, 1], {"x": xm})

    def token_x(q):
        gg = order[q]
        landed(token(gg, xm), tsem.at[gg, xm])
        if q % 2 == 0:
            push_token(gg, xm, ts_r.at[q], {"x": xp})
        landed(token(gg, xp), tsem.at[gg, xp])
        if q % 2 == 1:
            push_token(gg, xp, ts_r.at[q], {"x": xm})

    def token_far(q):
        gg = order[q]
        landed(token(gg, xf), tsem.at[gg, xf])

    def weight_y(i):
        gg = kinds[1]
        landed(weight(z, gg, i), wsem.at[z, gg, i])
        push_weight(z, gg, i, ws_b.at[i, 0], {"z": zp})
        push_weight(z, gg, i, ws_b.at[i, 1], {"z": zm})
        push_weight(z, gg, i, ws_b.at[i, 2], sibling)

    def weight_z(kind, i):
        gg = kinds[kind]
        landed(weight(zm, gg, i), wsem.at[zm, gg, i])
        if i % 2 == 0:
            push_weight(zm, gg, i, ws_r.at[kind, i], {"z": zp})
        push_weight(zm, gg, i, ws_n.at[0, kind, i], sibling)
        landed(weight(zp, gg, i), wsem.at[zp, gg, i])
        if i % 2 == 1:
            push_weight(zp, gg, i, ws_r.at[kind, i], {"z": zm})
        push_weight(zp, gg, i, ws_n.at[1, kind, i], sibling)

    def weight_far(kind, i):
        gg = kinds[kind]
        landed(weight(zf, gg, i), wsem.at[zf, gg, i])
        push_weight(zf, gg, i, ws_f.at[kind, i], sibling)

    def from_sibling(zz):
        for hh in (0, 1):
            for i in range(4):
                gg = 2 * hh + other
                landed(weight(zz, gg, i), wsem.at[zz, gg, i])

    def out_slot(ll, hh):
        return o_ref.at[:, pl.ds(pl.multiple_of((2 * ll + hh) * S, S), S)]

    def out_remote(zz, k):
        return pltpu.make_async_remote_copy(
            src_ref=O.at[k], dst_ref=out_slot(l, h), send_sem=os.at[k], recv_sem=osem.at[2 * l + h],
            device_id={"l": c, "h": zz // 2, "c": zz % 2}, device_id_type=MESH,
        )

    def out_local(k):
        return pltpu.make_async_copy(O.at[k], out_slot(l, h), osem.at[2 * l + h])

    def mine(zz):
        return jnp.logical_and(c == l, zz == g)

    def columns(zz, k):
        which = 2 * ((zz // 2 + h) % 2) + (zz % 2 + c) % 2
        bias = B[which, :, pl.ds(pl.multiple_of((2 * l + h) * S, S), S)]

        @pl.loop(0, ROWS // TILE)
        def _(m):
            rows = pl.ds(pl.multiple_of(m * TILE, TILE), TILE)
            pre = jnp.dot(T[rows, :], W[zz], preferred_element_type=jnp.float32) + bias
            act = pre * (1.0 + lax.erf(pre * 0.7071067811865476)) * 0.5
            O[k, rows, :] = act.astype(jnp.bfloat16)

        @pl.when(mine(zz))
        def _():
            out_local(k).start()

        @pl.when(jnp.logical_not(mine(zz)))
        def _():
            out_remote(zz, k).start()

    token_y(0)
    token_y(1)
    weight_z(0, 0)
    token_y(2)
    token_y(3)
    weight_z(0, 1)
    weight_y(0)
    token_x(0)
    weight_z(0, 2)
    token_x(1)
    weight_y(1)
    weight_z(0, 3)
    token_x(2)
    weight_y(2)
    weight_z(1, 0)
    token_x(3)
    weight_y(3)
    weight_z(1, 1)
    weight_z(1, 2)
    for i in range(4):
        landed(weight(z, g, i), wsem.at[z, g, i])
    landed(B.at[0], bsem.at[0])
    for k in range(3):
        landed(B.at[1 + k], bsem.at[1 + k])
    for q in range(4):
        token_far(q)
    from_sibling(z)
    columns(z, 0)
    weight_z(1, 3)
    from_sibling(zm)
    columns(zm, 1)
    for i in range(4):
        weight_far(0, i)
    from_sibling(zp)
    columns(zp, 2)
    for i in range(4):
        weight_far(1, i)
    from_sibling(zf)
    columns(zf, 3)

    for ll in (0, 1):
        for hh in (0, 1):
            landed(out_slot(ll, hh), osem.at[2 * ll + hh])

    for copy in sends:
        copy.wait_send()

    @pl.when(c != l)
    def _():
        to_own_chip().wait_send()

    for k, zz in enumerate((z, zm, zp, zf)):
        @pl.when(jnp.logical_not(mine(zz)))
        def _():
            out_remote(zz, k).wait_send()


def per_device(tokens, weight, bias):
    any_spec = pl.BlockSpec(memory_space=pl.ANY)
    dma = pltpu.SemaphoreType.DMA
    return pl.pallas_call(
        kernel,
        out_shape=jax.ShapeDtypeStruct((ROWS, 4 * S), jnp.bfloat16),
        in_specs=[any_spec] * 3,
        out_specs=any_spec,
        scratch_shapes=[
            pltpu.VMEM((ROWS, D), jnp.bfloat16),
            pltpu.VMEM((4, D, S), jnp.bfloat16),
            pltpu.VMEM((4, 1, 4 * S), jnp.float32),
            pltpu.VMEM((4, ROWS, S), jnp.bfloat16),
            dma((4, 4)), dma((4, 4, 4)), dma((4,)), dma((4,)),
            dma((4,)), dma((4, 2)), dma((4,)), dma((4, 4)), dma((4, 3)),
            dma((2, 2, 4)), dma((2, 4)), dma((2, 4)), dma((3,)), dma((4,)),
        ],
        compiler_params=pltpu.CompilerParams(
            collective_id=0, has_side_effects=True, vmem_limit_bytes=60 * 2**20
        ),
    )(tokens, weight, bias.reshape(1, 4 * S))


def solution(mesh):
    torus = Mesh(mesh.devices.reshape(4, 4, 2, 2, 2), ("x", "z", "l", "h", "c"))
    placed = (P(("z", "l"), ("h", "c", "x")), P(("h", "c"), ("x", "z", "l")), P(("x", "h", "c")))
    return jax.shard_map(
        per_device, mesh=torus, in_specs=placed, out_specs=P(("z", "l"), ("x", "h", "c")), check_vma=False
    )
```

```python
import jax
import jax.numpy as jnp
from jax import lax
from jax.experimental import pallas as pl
from jax.experimental.pallas import tpu as pltpu
from jax.sharding import Mesh
from jax.sharding import PartitionSpec as P

MESH = pl.DeviceIdType.MESH
S = 384
ROWS = 512
D = 6144
TILE = 256
C = 128
QUARTER = 1536


def kernel(
    t_ref, w_ref, b_ref, o_ref,
    T, W, B, O,
    tsem, wsem, bsem, osem,
    ts_y, ts_x, ts_r, ws_a, ws_b, ws_n, ws_r, ws_f, bs, os,
):
    x, z, l, h, c = (lax.axis_index(a) for a in ("x", "z", "l", "h", "c"))
    y = 2 * h + l
    g = 2 * h + c
    other = 1 - c
    xp, xm, xf = (x + 1) % 4, (x + 3) % 4, (x + 2) % 4
    zp, zm, zf = (z + 1) % 4, (z + 3) % 4, (z + 2) % 4
    yp, ym = (y + 1) % 4, (y + 3) % 4
    order = [2 * hh + cc for hh in (h, 1 - h) for cc in (0, 1)]
    kinds = [g, 2 * (1 - h) + c]
    sibling = {"c": other}
    sends = []

    def token(gg, xx):
        return T.at[:, pl.ds(pl.multiple_of((gg * 4 + xx) * S, S), S)]

    def weight(zz, gg, i):
        return W.at[zz, pl.ds(pl.multiple_of(gg * QUARTER, QUARTER), QUARTER), pl.ds(i * C, C)]

    def shard(i, half):
        return w_ref.at[:, pl.ds(pl.multiple_of(half * S + i * C, C), C)]

    def push(src, dst, send, recv, to):
        copy = pltpu.make_async_remote_copy(
            src_ref=src, dst_ref=dst, send_sem=send, recv_sem=recv,
            device_id=to, device_id_type=MESH,
        )
        copy.start()
        sends.append(copy)

    def landed(slot, sem):
        pltpu.make_async_copy(slot, slot, sem).wait()

    def push_token(gg, xx, send, to):
        push(token(gg, xx), token(gg, xx), send, tsem.at[gg, xx], to)

    def push_weight(zz, gg, i, send, to):
        push(weight(zz, gg, i), weight(zz, gg, i), send, wsem.at[zz, gg, i], to)

    @pl.when(c == l)
    def _():
        pltpu.make_async_copy(t_ref, token(g, x), tsem.at[g, x]).start()

    for i in range(3):
        pltpu.make_async_copy(shard(i, h), weight(z, g, i), wsem.at[z, g, i]).start()
    pltpu.make_async_copy(b_ref, B.at[0], bsem.at[0]).start()

    barrier = pltpu.get_barrier_semaphore()
    peers = [
        {"l": (l + dl) % 2, "h": (h + dh) % 2, "c": (c + dc) % 2}
        for dl in (0, 1) for dh in (0, 1) for dc in (0, 1) if dl + dh + dc
    ]
    peers += [{"x": xp}, {"x": xm}, {"z": zp}, {"z": zm}]
    for peer in peers:
        pl.semaphore_signal(barrier, inc=1, device_id=peer, device_id_type=MESH)
    pl.semaphore_wait(barrier, len(peers))

    def to_own_chip():
        return pltpu.make_async_remote_copy(
            src_ref=t_ref, dst_ref=token(g, x), send_sem=ts_y.at[3], recv_sem=tsem.at[g, x],
            device_id=sibling, device_id_type=MESH,
        )

    @pl.when(c != l)
    def _():
        to_own_chip().start()

    for k, yy in enumerate((yp, ym, (y + 2) % 4)):
        push(t_ref, token(g, x), ts_y.at[k], tsem.at[g, x], {"l": yy % 2, "h": yy // 2, "c": l})
    for i in range(3):
        push(shard(i, h), weight(z, g, i), ws_a.at[i, 0], wsem.at[z, g, i], {"z": zp})
        push(shard(i, h), weight(z, g, i), ws_a.at[i, 1], wsem.at[z, g, i], {"z": zm})
        push(shard(i, 1 - h), weight(z, g, i), ws_a.at[i, 3], wsem.at[z, g, i], {"h": 1 - h})
        push(shard(i, h), weight(z, g, i), ws_a.at[i, 2], wsem.at[z, g, i], sibling)
    for k, (dh, dc) in enumerate(((0, 1), (1, 0), (1, 1))):
        to = {"h": (h + dh) % 2, "c": (c + dc) % 2}
        push(b_ref, B.at[1 + k], bs.at[k], bsem.at[1 + k], to)

    def token_y(q):
        gg = order[q]
        landed(token(gg, x), tsem.at[gg, x])
        push_token(gg, x, ts_x.at[q, 0], {"x": xp})
        push_token(gg, x, ts_x.at[q, 1], {"x": xm})

    def token_x(q):
        gg = order[q]
        landed(token(gg, xm), tsem.at[gg, xm])
        if q % 2 == 0:
            push_token(gg, xm, ts_r.at[q], {"x": xp})
        landed(token(gg, xp), tsem.at[gg, xp])
        if q % 2 == 1:
            push_token(gg, xp, ts_r.at[q], {"x": xm})

    def token_far(q):
        gg = order[q]
        landed(token(gg, xf), tsem.at[gg, xf])

    def weight_y(i):
        gg = kinds[1]
        landed(weight(z, gg, i), wsem.at[z, gg, i])
        push_weight(z, gg, i, ws_b.at[i, 0], {"z": zp})
        push_weight(z, gg, i, ws_b.at[i, 1], {"z": zm})
        push_weight(z, gg, i, ws_b.at[i, 2], sibling)

    def weight_z(kind, i):
        gg = kinds[kind]
        landed(weight(zm, gg, i), wsem.at[zm, gg, i])
        push_weight(zm, gg, i, ws_n.at[0, kind, i], sibling)
        landed(weight(zp, gg, i), wsem.at[zp, gg, i])
        push_weight(zp, gg, i, ws_n.at[1, kind, i], sibling)

    def relay(kind, i):
        if kind == 0:
            push_weight(zm, kinds[0], i, ws_r.at[0, i], {"z": zp})
        else:
            push_weight(zp, kinds[1], i, ws_r.at[1, i], {"z": zm})

    def weight_far(kind, i):
        gg = kinds[kind]
        landed(weight(zf, gg, i), wsem.at[zf, gg, i])
        push_weight(zf, gg, i, ws_f.at[kind, i], sibling)

    def from_sibling(zz, i):
        for hh in (0, 1):
            gg = 2 * hh + other
            landed(weight(zz, gg, i), wsem.at[zz, gg, i])

    def out_slot(ll, hh, first=0, width=S):
        return o_ref.at[:, pl.ds(pl.multiple_of((2 * ll + hh) * S + first, C), width)]

    def out_remote(zz, k, first, width):
        return pltpu.make_async_remote_copy(
            src_ref=O.at[k, :, pl.ds(first, width)], dst_ref=out_slot(l, h, first, width),
            send_sem=os.at[k, first // C], recv_sem=osem.at[2 * l + h],
            device_id={"l": c, "h": zz // 2, "c": zz % 2}, device_id_type=MESH,
        )

    def out_local(k, first, width):
        return pltpu.make_async_copy(
            O.at[k, :, pl.ds(first, width)], out_slot(l, h, first, width), osem.at[2 * l + h]
        )

    def mine(zz):
        return jnp.logical_and(c == l, zz == g)

    def columns(zz, k, first=0, width=S):
        which = 2 * ((zz // 2 + h) % 2) + (zz % 2 + c) % 2
        parts = [
            B[which, pl.ds((2 * l + h) * 3 + t, 1), :] for t in range(first // C, (first + width) // C)
        ]
        bias = jnp.concatenate(parts, axis=1) if len(parts) > 1 else parts[0]

        @pl.loop(0, ROWS // TILE)
        def _(m):
            rows = pl.ds(pl.multiple_of(m * TILE, TILE), TILE)
            pre = jnp.dot(
                T[rows, :], W[zz, :, pl.ds(first, width)], preferred_element_type=jnp.float32
            ) + bias
            act = pre * (1.0 + lax.erf(pre * 0.7071067811865476)) * 0.5
            O[k, rows, pl.ds(first, width)] = act.astype(jnp.bfloat16)

        @pl.when(mine(zz))
        def _():
            out_local(k, first, width).start()

        @pl.when(jnp.logical_not(mine(zz)))
        def _():
            out_remote(zz, k, first, width).start()

    token_y(0)
    token_y(1)
    weight_z(0, 0)
    weight_y(0)
    token_y(2)
    token_y(3)
    weight_z(0, 1)
    weight_y(1)
    token_x(0)
    weight_z(0, 2)
    token_x(1)
    weight_y(2)
    for i in range(3):
        relay(0, i)
    weight_z(1, 0)
    relay(1, 0)
    token_x(2)
    weight_z(1, 1)
    relay(1, 1)
    token_x(3)
    weight_z(1, 2)
    relay(1, 2)
    for i in range(3):
        landed(weight(z, g, i), wsem.at[z, g, i])
    landed(B.at[0], bsem.at[0])
    for k in range(3):
        landed(B.at[1 + k], bsem.at[1 + k])
    for q in range(4):
        token_far(q)
    for i in range(3):
        from_sibling(z, i)
    columns(z, 0)
    for i in range(3):
        from_sibling(zm, i)
    columns(zm, 1)
    weight_far(0, 0)
    weight_far(1, 0)
    for i in range(3):
        from_sibling(zp, i)
    columns(zp, 2)
    for i in range(3):
        if i:
            weight_far(0, i)
            weight_far(1, i)
        from_sibling(zf, i)
        columns(zf, 3, i * C, C)

    for ll in (0, 1):
        for hh in (0, 1):
            landed(out_slot(ll, hh), osem.at[2 * ll + hh])

    for copy in sends:
        copy.wait_send()

    @pl.when(c != l)
    def _():
        to_own_chip().wait_send()

    whole = [(zz, k, 0, S) for k, zz in enumerate((z, zm, zp))]
    for zz, *where in whole + [(zf, 3, i * C, C) for i in range(3)]:
        @pl.when(jnp.logical_not(mine(zz)))
        def _():
            out_remote(zz, *where).wait_send()


def per_device(tokens, weight, bias):
    any_spec = pl.BlockSpec(memory_space=pl.ANY)
    dma = pltpu.SemaphoreType.DMA
    return pl.pallas_call(
        kernel,
        out_shape=jax.ShapeDtypeStruct((ROWS, 4 * S), jnp.bfloat16),
        in_specs=[pl.BlockSpec(memory_space=pltpu.HBM)] * 3,
        out_specs=any_spec,
        scratch_shapes=[
            pltpu.VMEM((ROWS, D), jnp.bfloat16),
            pltpu.VMEM((4, D, S), jnp.bfloat16),
            pltpu.VMEM((4, 12, C), jnp.float32),
            pltpu.VMEM((4, ROWS, S), jnp.bfloat16),
            dma((4, 4)), dma((4, 4, 3)), dma((4,)), dma((4,)),
            dma((4,)), dma((4, 2)), dma((4,)), dma((3, 4)), dma((3, 3)),
            dma((2, 2, 3)), dma((2, 3)), dma((2, 3)), dma((3,)), dma((4, 3)),
        ],
        compiler_params=pltpu.CompilerParams(
            collective_id=0, has_side_effects=True, vmem_limit_bytes=48 * 2**20
        ),
    )(*(pltpu.with_memory_space_constraint(a, pltpu.HBM) for a in (tokens, weight, bias.reshape(12, C))))


def solution(mesh):
    torus = Mesh(mesh.devices.reshape(4, 4, 2, 2, 2), ("x", "z", "l", "h", "c"))
    placed = (P(("z", "l"), ("h", "c", "x")), P(("h", "c"), ("x", "z", "l")), P(("x", "h", "c")))
    return jax.shard_map(
        per_device, mesh=torus, in_specs=placed, out_specs=P(("z", "l"), ("x", "h", "c")), check_vma=False
    )
```

```python
import jax
import jax.numpy as jnp
from jax import lax
from jax.experimental import pallas as pl
from jax.experimental.pallas import tpu as pltpu
from jax.sharding import Mesh
from jax.sharding import PartitionSpec as P

MESH = pl.DeviceIdType.MESH
S = 384
C = 128
ROWS = 512
D = 6144
TILE = 256

PAIR = 2 * S
HALF = 4 * PAIR


def kernel(
    t_ref, w_ref, b_ref, o_ref,
    T, W, G, B, A, O,
    lsem, tsem, wsem, bsem, osem,
    ts_y, ts_x, ts_r, ws_a, ws_b, ws_n, ws_r, ws_f, bs, os,
):
    x, z, l, h, c = (lax.axis_index(a) for a in ("x", "z", "l", "h", "c"))
    y = 2 * h + l
    g = 2 * h + c
    other = 1 - c
    xp, xm = (x + 1) % 4, (x + 3) % 4
    zp, zm, zf = (z + 1) % 4, (z + 3) % 4, (z + 2) % 4
    yp, ym = (y + 1) % 4, (y + 3) % 4
    sibling = {"c": other}
    sends = []

    def half_rows(part):
        return pl.ds(part * TILE, TILE)

    def token(hk, r, cc, part):
        return T.at[half_rows(part), pl.ds(pl.multiple_of(hk * HALF + r * PAIR + cc * S, S), S)]

    def weight(zz, hk, cc, i):
        if zz is zf and i >= 2:
            return W.at[zz, hk, pl.ds(2 * (i - 2), 2), cc, :, pl.ds(2 * C, C)]
        return W.at[zz, hk, :, cc, :, pl.ds(i * C, C)]

    def push(src, dst, send, recv, to):
        copy = pltpu.make_async_remote_copy(
            src_ref=src, dst_ref=dst, send_sem=send, recv_sem=recv,
            device_id=to, device_id_type=MESH,
        )
        copy.start()
        sends.append(copy)

    def landed(slot, sem):
        pltpu.make_async_copy(slot, slot, sem).wait()

    def push_token(q, r, r_there, part, send, to):
        hk, cc = divmod(q, 2)
        push(token(hk, r, cc, part), token(hk, r_there, cc, part), send, tsem.at[hk, r_there, cc, part], to)

    def push_weight(zz, kind, i, send, to):
        push(weight(zz, kind, c, i), weight(zz, kind, c, i), send, wsem.at[zz, kind, c, i], to)

    @pl.when(c == l)
    def _():
        for part in (0, 1):
            pltpu.make_async_copy(t_ref.at[half_rows(part)], token(0, 1, c, part), tsem.at[0, 1, c, part]).start()

    def stage(half, slot, row, k):
        src = w_ref.at[pl.ds(row * S, S), pl.ds(pl.multiple_of(half * S, S), S)]
        return pltpu.make_async_copy(src, slot, lsem.at[k, row])

    staged = [
        [stage(h, W.at[z, 0, (row - x + 5) % 4, c], row, 0) for row in range(4)],
        [stage(1 - h, G.at[(row - x + 5) % 4], row, 1) for row in range(4)],
    ]
    for copies in staged:
        for copy in copies:
            copy.start()
    pltpu.make_async_copy(b_ref, B.at[0], bsem.at[0]).start()

    barrier = pltpu.get_barrier_semaphore()
    peers = [
        {"l": (l + dl) % 2, "h": (h + dh) % 2, "c": (c + dc) % 2}
        for dl in (0, 1) for dh in (0, 1) for dc in (0, 1) if dl + dh + dc
    ]
    peers += [{"x": xp}, {"x": xm}, {"z": zp}, {"z": zm}]
    for peer in peers:
        pl.semaphore_signal(barrier, inc=1, device_id=peer, device_id_type=MESH)
    for copy in staged[0]:
        copy.wait()
    pl.semaphore_wait(barrier, len(peers))

    def to_own_chip(part):
        return pltpu.make_async_remote_copy(
            src_ref=t_ref.at[half_rows(part)], dst_ref=token(0, 1, c, part),
            send_sem=ts_y.at[3, part], recv_sem=tsem.at[0, 1, c, part],
            device_id=sibling, device_id_type=MESH,
        )

    @pl.when(c != l)
    def _():
        to_own_chip(0).start()
        to_own_chip(1).start()

    def token_column(part):
        for k, yy in enumerate((yp, ym, (y + 2) % 4)):
            hk = (yy // 2 + h) % 2
            push(
                t_ref.at[half_rows(part)], token(hk, 1, c, part), ts_y.at[k, part], tsem.at[hk, 1, c, part],
                {"l": yy % 2, "h": yy // 2, "c": l},
            )

    def weight_column(i):
        push(G.at[:, :, pl.ds(i * C, C)], weight(z, 1, c, i), ws_a.at[i, 3], wsem.at[z, 1, c, i], {"h": 1 - h})

    for i in range(3):
        push_weight(z, 0, i, ws_a.at[i, 0], {"z": zp})
        push_weight(z, 0, i, ws_a.at[i, 1], {"z": zm})
    token_column(0)
    for copy in staged[1]:
        copy.wait()
    weight_column(0)
    token_column(1)
    weight_column(1)
    weight_column(2)
    for i in range(3):
        push_weight(z, 0, i, ws_a.at[i, 2], sibling)
    for k, (dh, dc) in enumerate(((0, 1), (1, 0), (1, 1))):
        to = {"h": (h + dh) % 2, "c": (c + dc) % 2}
        push(b_ref, B.at[1 + k], bs.at[k], bsem.at[1 + k], to)

    def token_in(q, r, part):
        hk, cc = divmod(q, 2)
        landed(token(hk, r, cc, part), tsem.at[hk, r, cc, part])

    def token_y(q, part):
        token_in(q, 1, part)
        push_token(q, 1, 0, part, ts_x.at[q, 0, part], {"x": xp})
        push_token(q, 1, 2, part, ts_x.at[q, 1, part], {"x": xm})

    def token_x(q, part):
        token_in(q, 0, part)
        if q % 2 == 0:
            push_token(q, 0, 3, part, ts_r.at[q, part], {"x": xp})
        token_in(q, 2, part)
        if q % 2 == 1:
            push_token(q, 2, 3, part, ts_r.at[q, part], {"x": xm})

    def weight_in(zz, kind, cc, i):
        landed(weight(zz, kind, cc, i), wsem.at[zz, kind, cc, i])

    def weight_y(i):
        weight_in(z, 1, c, i)
        push_weight(z, 1, i, ws_b.at[i, 0], {"z": zp})
        push_weight(z, 1, i, ws_b.at[i, 1], {"z": zm})
        push_weight(z, 1, i, ws_b.at[i, 2], sibling)

    def weight_z(kind, i):
        weight_in(zm, kind, c, i)
        push_weight(zm, kind, i, ws_n.at[0, kind, i], sibling)
        weight_in(zp, kind, c, i)
        push_weight(zp, kind, i, ws_n.at[1, kind, i], sibling)

    def relay(kind, i):
        near, to = ((zm, zp), (zp, zm))[kind]

        def part(r, count):
            return W.at[near, kind, pl.ds(r, count), c, :, pl.ds(i * C, C)]

        for k, slot in enumerate([part(0, 4)] if i < 2 else [part(0, 2), part(2, 2)]):
            push(slot, slot, ws_r.at[kind, i + k], wsem.at[near, kind, c, i + k], {"z": to})

    def weight_far(kind, i):
        weight_in(zf, kind, c, i)
        push_weight(zf, kind, i, ws_f.at[kind, i], sibling)

    def from_sibling(zz):
        for kind in (0, 1):
            for i in range(3):
                weight_in(zz, kind, other, i)

    def out_slot(ll, hh, rows=pl.ds(0, ROWS), first=0, width=S):
        return o_ref.at[rows, pl.ds(pl.multiple_of((2 * ll + hh) * S + first, C), width)]

    def out_remote(zz, k, rows, first, width):
        return pltpu.make_async_remote_copy(
            src_ref=O.at[k, rows, pl.ds(first, width)], dst_ref=out_slot(l, h, rows, first, width),
            send_sem=os.at[k, first // C], recv_sem=osem.at[2 * l + h],
            device_id={"l": c, "h": zz // 2, "c": zz % 2}, device_id_type=MESH,
        )

    def out_local(k, rows, first, width):
        return pltpu.make_async_copy(
            O.at[k, rows, pl.ds(first, width)], out_slot(l, h, rows, first, width), osem.at[2 * l + h]
        )

    def mine(zz):
        return jnp.logical_and(c == l, zz == g)

    def dot(rows, start, count, w):
        return jnp.dot(
            T[rows, pl.ds(start, count)], w.reshape(count, w.shape[-1]), preferred_element_type=jnp.float32
        )

    def finish(zz, k, part, first, width, product):
        which = 2 * ((zz // 2 + h) % 2) + (zz % 2 + c) % 2
        parts = [
            B[which, pl.ds((2 * l + h) * 3 + t, 1), :] for t in range(first // C, (first + width) // C)
        ]
        bias = jnp.concatenate(parts, axis=1) if len(parts) > 1 else parts[0]
        rows = half_rows(part)
        pre = product + bias
        act = pre * (1.0 + lax.erf(pre * 0.7071067811865476)) * 0.5
        O[k, rows, pl.ds(first, width)] = act.astype(jnp.bfloat16)

        @pl.when(mine(zz))
        def _():
            out_local(k, rows, first, width).start()

        @pl.when(jnp.logical_not(mine(zz)))
        def _():
            out_remote(zz, k, rows, first, width).start()

    def columns(zz, k, part):
        finish(zz, k, part, 0, S, dot(half_rows(part), 0, D, W[zz]))

    def far_columns(i, part):
        finish(zf, 3, part, i * C, C, dot(half_rows(part), 0, D, W[zf, :, :, :, :, pl.ds(i * C, C)]))

    def last_columns(half, part):
        rows = half_rows(part)
        w = [W[zf, kind, pl.ds(2 * half, 2), :, :, pl.ds(2 * C, C)] for kind in (0, 1)]
        product = sum(dot(rows, kind * HALF + half * 2 * PAIR, 2 * PAIR, w[kind]) for kind in (0, 1))
        if half == 0:
            A[rows, :] = product
        else:
            finish(zf, 3, part, 2 * C, C, product + A[rows, :])

    for q in range(4):
        token_y(q, 0)
    weight_z(0, 0)
    token_x(0, 0)
    token_x(1, 0)
    token_y(0, 1)
    token_y(1, 1)
    token_x(2, 0)
    weight_z(0, 1)
    weight_y(0)
    token_x(3, 0)
    token_y(2, 1)
    token_y(3, 1)
    weight_z(0, 2)
    weight_y(1)
    token_x(0, 1)
    token_x(1, 1)
    weight_y(2)
    for i in range(3):
        relay(0, i)
    weight_z(1, 0)
    relay(1, 0)
    token_x(2, 1)
    weight_z(1, 1)
    relay(1, 1)
    token_x(3, 1)
    for k in range(4):
        landed(B.at[k], bsem.at[k])
    for q in range(4):
        token_in(q, 3, 0)
    from_sibling(z)
    columns(z, 0, 0)
    weight_z(1, 2)
    relay(1, 2)
    from_sibling(zm)
    columns(zm, 1, 0)
    from_sibling(zp)
    columns(zp, 2, 0)
    for q in range(4):
        token_in(q, 3, 1)
    columns(z, 0, 1)
    columns(zm, 1, 1)
    columns(zp, 2, 1)
    for i in range(4):
        for kind in (0, 1):
            weight_far(kind, i)
        for kind in (0, 1):
            weight_in(zf, kind, other, i)
        for part in (0, 1):
            if i < 2:
                far_columns(i, part)
            else:
                last_columns(i - 2, part)

    for ll in (0, 1):
        for hh in (0, 1):
            landed(out_slot(ll, hh), osem.at[2 * ll + hh])

    for copy in sends:
        copy.wait_send()

    @pl.when(c != l)
    def _():
        to_own_chip(0).wait_send()
        to_own_chip(1).wait_send()

    all_rows = pl.ds(0, ROWS)
    whole = [(zz, k, all_rows, 0, S) for k, zz in enumerate((z, zm, zp))]
    for zz, *where in whole + [(zf, 3, all_rows, i * C, C) for i in range(3)]:
        @pl.when(jnp.logical_not(mine(zz)))
        def _():
            out_remote(zz, *where).wait_send()


def per_device(tokens, weight, bias):
    any_spec = pl.BlockSpec(memory_space=pl.ANY)
    dma = pltpu.SemaphoreType.DMA
    in_hbm = [pltpu.with_memory_space_constraint(a, pltpu.HBM) for a in (tokens, weight, bias.reshape(12, C))]
    return pl.pallas_call(
        kernel,
        out_shape=jax.ShapeDtypeStruct((ROWS, 4 * S), jnp.bfloat16),
        in_specs=[pl.BlockSpec(memory_space=pltpu.HBM)] * 3,
        out_specs=any_spec,
        scratch_shapes=[
            pltpu.VMEM((ROWS, D), jnp.bfloat16),
            pltpu.VMEM((4, 2, 4, 2, S, S), jnp.bfloat16),
            pltpu.VMEM((4, S, S), jnp.bfloat16),
            pltpu.VMEM((4, 12, C), jnp.float32),
            pltpu.VMEM((ROWS, C), jnp.float32),
            pltpu.VMEM((4, ROWS, S), jnp.bfloat16),
            dma((2, 4)), dma((2, 4, 2, 2)), dma((4, 2, 2, 4)), dma((4,)), dma((4,)),
            dma((4, 2)), dma((4, 2, 2)), dma((4, 2)), dma((3, 4)), dma((3, 3)),
            dma((2, 2, 3)), dma((2, 4)), dma((2, 4)), dma((3,)), dma((4, 3)),
        ],
        compiler_params=pltpu.CompilerParams(
            collective_id=0, has_side_effects=True, vmem_limit_bytes=48 * 2**20
        ),
    )(*in_hbm)


def solution(mesh):
    torus = Mesh(mesh.devices.reshape(4, 4, 2, 2, 2), ("x", "z", "l", "h", "c"))
    placed = (P(("z", "l"), ("h", "c", "x")), P(("h", "c"), ("x", "z", "l")), P(("x", "h", "c")))
    return jax.shard_map(
        per_device, mesh=torus, in_specs=placed, out_specs=P(("z", "l"), ("x", "h", "c")), check_vma=False
    )
```

```python
import jax
import jax.numpy as jnp
from jax import lax
from jax.experimental import pallas as pl
from jax.experimental.pallas import tpu as pltpu
from jax.sharding import Mesh
from jax.sharding import PartitionSpec as P

MESH = pl.DeviceIdType.MESH
S = 384
C = 128
ROWS = 512
D = 6144
TILE = 256

PAIR = 2 * S
HALF = 4 * PAIR


def kernel(
    t_ref, w_ref, b_ref, o_ref,
    T, W, G, B, A, O,
    lsem, tsem, wsem, bsem, osem,
    ts_y, ts_x, ts_r, ws_a, ws_b, ws_n, ws_r, ws_f, bs, os,
):
    x, z, l, h, c = (lax.axis_index(a) for a in ("x", "z", "l", "h", "c"))
    y = 2 * h + l
    g = 2 * h + c
    other = 1 - c
    xp, xm = (x + 1) % 4, (x + 3) % 4
    zp, zm, zf = (z + 1) % 4, (z + 3) % 4, (z + 2) % 4
    yp, ym = (y + 1) % 4, (y + 3) % 4
    sibling = {"c": other}
    sends = []

    def half_rows(part):
        return pl.ds(part * TILE, TILE)

    def token(hk, r, cc, part):
        return T.at[half_rows(part), pl.ds(pl.multiple_of(hk * HALF + r * PAIR + cc * S, S), S)]

    def weight(zz, hk, cc, i):
        if zz is zf and i >= 2:
            return W.at[zz, hk, pl.ds(2 * (i - 2), 2), cc, :, pl.ds(2 * C, C)]
        return W.at[zz, hk, :, cc, :, pl.ds(i * C, C)]

    def push(src, dst, send, recv, to):
        copy = pltpu.make_async_remote_copy(
            src_ref=src, dst_ref=dst, send_sem=send, recv_sem=recv,
            device_id=to, device_id_type=MESH,
        )
        copy.start()
        sends.append(copy)

    def landed(slot, sem):
        pltpu.make_async_copy(slot, slot, sem).wait()

    def push_token(q, r, r_there, part, send, to):
        hk, cc = divmod(q, 2)
        push(token(hk, r, cc, part), token(hk, r_there, cc, part), send, tsem.at[hk, r_there, cc, part], to)

    def push_weight(zz, kind, i, send, to):
        push(weight(zz, kind, c, i), weight(zz, kind, c, i), send, wsem.at[zz, kind, c, i], to)

    @pl.when(c == l)
    def _():
        for part in (0, 1):
            pltpu.make_async_copy(t_ref.at[half_rows(part)], token(0, 1, c, part), tsem.at[0, 1, c, part]).start()

    def stage(half, slot, row, k):
        src = w_ref.at[pl.ds(row * S, S), pl.ds(pl.multiple_of(half * S, S), S)]
        return pltpu.make_async_copy(src, slot, lsem.at[k, row])

    staged = [
        [stage(h, W.at[z, 0, (row - x + 5) % 4, c], row, 0) for row in range(4)],
        [stage(1 - h, G.at[(row - x + 5) % 4], row, 1) for row in range(4)],
    ]
    for copies in staged:
        for copy in copies:
            copy.start()
    pltpu.make_async_copy(b_ref, B.at[0], bsem.at[0]).start()

    barrier = pltpu.get_barrier_semaphore()
    peers = [
        {"l": (l + dl) % 2, "h": (h + dh) % 2, "c": (c + dc) % 2}
        for dl in (0, 1) for dh in (0, 1) for dc in (0, 1) if dl + dh + dc
    ]
    peers += [{"x": xp}, {"x": xm}, {"z": zp}, {"z": zm}]
    for peer in peers:
        pl.semaphore_signal(barrier, inc=1, device_id=peer, device_id_type=MESH)
    for copy in staged[0]:
        copy.wait()
    pl.semaphore_wait(barrier, len(peers))

    def to_own_chip(part):
        return pltpu.make_async_remote_copy(
            src_ref=t_ref.at[half_rows(part)], dst_ref=token(0, 1, c, part),
            send_sem=ts_y.at[3, part], recv_sem=tsem.at[0, 1, c, part],
            device_id=sibling, device_id_type=MESH,
        )

    @pl.when(c != l)
    def _():
        to_own_chip(0).start()
        to_own_chip(1).start()

    def token_column(part, steps=(0, 1, 2)):
        for k in steps:
            yy = (yp, ym, (y + 2) % 4)[k]
            hk = (yy // 2 + h) % 2
            push(
                t_ref.at[half_rows(part)], token(hk, 1, c, part), ts_y.at[k, part], tsem.at[hk, 1, c, part],
                {"l": yy % 2, "h": yy // 2, "c": l},
            )

    def weight_column(i):
        push(G.at[:, :, pl.ds(i * C, C)], weight(z, 1, c, i), ws_a.at[i, 3], wsem.at[z, 1, c, i], {"h": 1 - h})

    for i in range(3):
        push_weight(z, 0, i, ws_a.at[i, 0], {"z": zp})
        push_weight(z, 0, i, ws_a.at[i, 1], {"z": zm})
    token_column(0)
    for copy in staged[1]:
        copy.wait()
    weight_column(0)
    token_column(1, (0, 1))
    weight_column(1)
    weight_column(2)
    token_column(1, (2,))
    for i in range(3):
        push_weight(z, 0, i, ws_a.at[i, 2], sibling)
    for k, (dh, dc) in enumerate(((0, 1), (1, 0), (1, 1))):
        to = {"h": (h + dh) % 2, "c": (c + dc) % 2}
        push(b_ref, B.at[1 + k], bs.at[k], bsem.at[1 + k], to)

    def token_in(q, r, part):
        hk, cc = divmod(q, 2)
        landed(token(hk, r, cc, part), tsem.at[hk, r, cc, part])

    def token_y(q, part):
        token_in(q, 1, part)
        push_token(q, 1, 0, part, ts_x.at[q, 0, part], {"x": xp})
        push_token(q, 1, 2, part, ts_x.at[q, 1, part], {"x": xm})

    def token_x(q, part):
        token_in(q, 0, part)
        if q % 2 == 0:
            push_token(q, 0, 3, part, ts_r.at[q, part], {"x": xp})
        token_in(q, 2, part)
        if q % 2 == 1:
            push_token(q, 2, 3, part, ts_r.at[q, part], {"x": xm})

    def weight_in(zz, kind, cc, i):
        landed(weight(zz, kind, cc, i), wsem.at[zz, kind, cc, i])

    def weight_y(i):
        weight_in(z, 1, c, i)
        push_weight(z, 1, i, ws_b.at[i, 0], {"z": zp})
        push_weight(z, 1, i, ws_b.at[i, 1], {"z": zm})
        push_weight(z, 1, i, ws_b.at[i, 2], sibling)

    def weight_z(kind, i):
        weight_in(zm, kind, c, i)
        push_weight(zm, kind, i, ws_n.at[0, kind, i], sibling)
        weight_in(zp, kind, c, i)
        push_weight(zp, kind, i, ws_n.at[1, kind, i], sibling)

    def relay(kind, i):
        near, to = ((zm, zp), (zp, zm))[kind]

        def part(r, count):
            return W.at[near, kind, pl.ds(r, count), c, :, pl.ds(i * C, C)]

        for k, slot in enumerate([part(0, 4)] if i < 2 else [part(0, 2), part(2, 2)]):
            push(slot, slot, ws_r.at[kind, i + k], wsem.at[near, kind, c, i + k], {"z": to})

    def weight_far(kind, i):
        weight_in(zf, kind, c, i)
        push_weight(zf, kind, i, ws_f.at[kind, i], sibling)

    def from_sibling(zz):
        for kind in (0, 1):
            for i in range(3):
                weight_in(zz, kind, other, i)

    def out_slot(ll, hh, rows=pl.ds(0, ROWS), first=0, width=S):
        return o_ref.at[rows, pl.ds(pl.multiple_of((2 * ll + hh) * S + first, C), width)]

    def out_remote(zz, k, rows, first, width):
        return pltpu.make_async_remote_copy(
            src_ref=O.at[k, rows, pl.ds(first, width)], dst_ref=out_slot(l, h, rows, first, width),
            send_sem=os.at[k, first // C], recv_sem=osem.at[2 * l + h],
            device_id={"l": c, "h": zz // 2, "c": zz % 2}, device_id_type=MESH,
        )

    def out_local(k, rows, first, width):
        return pltpu.make_async_copy(
            O.at[k, rows, pl.ds(first, width)], out_slot(l, h, rows, first, width), osem.at[2 * l + h]
        )

    def mine(zz):
        return jnp.logical_and(c == l, zz == g)

    def dot(rows, start, count, w):
        return jnp.dot(
            T[rows, pl.ds(start, count)], w.reshape(count, w.shape[-1]), preferred_element_type=jnp.float32
        )

    def finish(zz, k, part, first, width, product):
        which = 2 * ((zz // 2 + h) % 2) + (zz % 2 + c) % 2
        parts = [
            B[which, pl.ds((2 * l + h) * 3 + t, 1), :] for t in range(first // C, (first + width) // C)
        ]
        bias = jnp.concatenate(parts, axis=1) if len(parts) > 1 else parts[0]
        rows = half_rows(part)
        pre = product + bias
        act = pre * (1.0 + lax.erf(pre * 0.7071067811865476)) * 0.5
        O[k, rows, pl.ds(first, width)] = act.astype(jnp.bfloat16)

        @pl.when(mine(zz))
        def _():
            out_local(k, rows, first, width).start()

        @pl.when(jnp.logical_not(mine(zz)))
        def _():
            out_remote(zz, k, rows, first, width).start()

    def columns(zz, k, part):
        finish(zz, k, part, 0, S, dot(half_rows(part), 0, D, W[zz]))

    def far_columns(i, part):
        finish(zf, 3, part, i * C, C, dot(half_rows(part), 0, D, W[zf, :, :, :, :, pl.ds(i * C, C)]))

    def last_columns(half, part):
        rows = half_rows(part)
        w = [W[zf, kind, pl.ds(2 * half, 2), :, :, pl.ds(2 * C, C)] for kind in (0, 1)]
        product = sum(dot(rows, kind * HALF + half * 2 * PAIR, 2 * PAIR, w[kind]) for kind in (0, 1))
        if half == 0:
            A[rows, :] = product
        else:
            finish(zf, 3, part, 2 * C, C, product + A[rows, :])

    for q in range(4):
        token_y(q, 0)
    weight_z(0, 0)
    token_x(0, 0)
    token_x(1, 0)
    weight_y(0)
    weight_z(0, 1)
    token_x(2, 0)
    token_x(3, 0)
    token_y(0, 1)
    token_y(1, 1)
    weight_z(0, 2)
    weight_y(1)
    weight_z(1, 0)
    token_x(0, 1)
    weight_y(2)
    for i in range(3):
        relay(0, i)
    relay(1, 0)
    token_x(1, 1)
    token_y(2, 1)
    token_y(3, 1)
    weight_z(1, 1)
    relay(1, 1)
    token_x(2, 1)
    token_x(3, 1)
    for k in range(4):
        landed(B.at[k], bsem.at[k])
    for q in range(4):
        token_in(q, 3, 0)
    from_sibling(z)
    columns(z, 0, 0)
    weight_z(1, 2)
    relay(1, 2)
    from_sibling(zm)
    columns(zm, 1, 0)
    from_sibling(zp)
    columns(zp, 2, 0)
    for q in range(4):
        token_in(q, 3, 1)
    columns(z, 0, 1)
    columns(zm, 1, 1)
    columns(zp, 2, 1)
    for i in range(4):
        for kind in (0, 1):
            weight_far(kind, i)
        for kind in (0, 1):
            weight_in(zf, kind, other, i)
        for part in (0, 1):
            if i < 2:
                far_columns(i, part)
            else:
                last_columns(i - 2, part)

    for ll in (0, 1):
        for hh in (0, 1):
            landed(out_slot(ll, hh), osem.at[2 * ll + hh])

    for copy in sends:
        copy.wait_send()

    @pl.when(c != l)
    def _():
        to_own_chip(0).wait_send()
        to_own_chip(1).wait_send()

    all_rows = pl.ds(0, ROWS)
    whole = [(zz, k, all_rows, 0, S) for k, zz in enumerate((z, zm, zp))]
    for zz, *where in whole + [(zf, 3, all_rows, i * C, C) for i in range(3)]:
        @pl.when(jnp.logical_not(mine(zz)))
        def _():
            out_remote(zz, *where).wait_send()


def per_device(tokens, weight, bias):
    any_spec = pl.BlockSpec(memory_space=pl.ANY)
    dma = pltpu.SemaphoreType.DMA
    in_hbm = [pltpu.with_memory_space_constraint(a, pltpu.HBM) for a in (tokens, weight, bias.reshape(12, C))]
    return pl.pallas_call(
        kernel,
        out_shape=jax.ShapeDtypeStruct((ROWS, 4 * S), jnp.bfloat16),
        in_specs=[pl.BlockSpec(memory_space=pltpu.HBM)] * 3,
        out_specs=any_spec,
        scratch_shapes=[
            pltpu.VMEM((ROWS, D), jnp.bfloat16),
            pltpu.VMEM((4, 2, 4, 2, S, S), jnp.bfloat16),
            pltpu.VMEM((4, S, S), jnp.bfloat16),
            pltpu.VMEM((4, 12, C), jnp.float32),
            pltpu.VMEM((ROWS, C), jnp.float32),
            pltpu.VMEM((4, ROWS, S), jnp.bfloat16),
            dma((2, 4)), dma((2, 4, 2, 2)), dma((4, 2, 2, 4)), dma((4,)), dma((4,)),
            dma((4, 2)), dma((4, 2, 2)), dma((4, 2)), dma((3, 4)), dma((3, 3)),
            dma((2, 2, 3)), dma((2, 4)), dma((2, 4)), dma((3,)), dma((4, 3)),
        ],
        compiler_params=pltpu.CompilerParams(
            collective_id=0, has_side_effects=True, vmem_limit_bytes=48 * 2**20
        ),
    )(*in_hbm)


def solution(mesh):
    torus = Mesh(mesh.devices.reshape(4, 4, 2, 2, 2), ("x", "z", "l", "h", "c"))
    placed = (P(("z", "l"), ("h", "c", "x")), P(("h", "c"), ("x", "z", "l")), P(("x", "h", "c")))
    return jax.shard_map(
        per_device, mesh=torus, in_specs=placed, out_specs=P(("z", "l"), ("x", "h", "c")), check_vma=False
    )
```

```python
import jax
import jax.numpy as jnp
from jax import lax
from jax.experimental import pallas as pl
from jax.experimental.pallas import tpu as pltpu
from jax.sharding import Mesh
from jax.sharding import PartitionSpec as P

MESH = pl.DeviceIdType.MESH
S = 384
C = 128
ROWS = 512
D = 6144
TILE = 256

PAIR = 2 * S
HALF = 4 * PAIR


def kernel(
    t_ref, w_ref, b_ref, o_ref,
    T, W, G, B, A, O,
    lsem, tsem, wsem, bsem, osem,
    ts_y, ts_x, ts_r, ws_a, ws_b, ws_n, ws_r, ws_f, bs, os,
):
    x, z, l, h, c = (lax.axis_index(a) for a in ("x", "z", "l", "h", "c"))
    y = 2 * h + l
    g = 2 * h + c
    other = 1 - c
    xp, xm = (x + 1) % 4, (x + 3) % 4
    zp, zm, zf = (z + 1) % 4, (z + 3) % 4, (z + 2) % 4
    yp, ym = (y + 1) % 4, (y + 3) % 4
    sibling = {"c": other}
    sends = []

    def half_rows(part):
        return pl.ds(part * TILE, TILE)

    def token(hk, r, cc, part):
        return T.at[half_rows(part), pl.ds(pl.multiple_of(hk * HALF + r * PAIR + cc * S, S), S)]

    def weight(zz, hk, cc, i):
        if zz is zf and i >= 2:
            return W.at[zz, hk, pl.ds(2 * (i - 2), 2), cc, :, pl.ds(2 * C, C)]
        return W.at[zz, hk, :, cc, :, pl.ds(i * C, C)]

    def push(src, dst, send, recv, to):
        copy = pltpu.make_async_remote_copy(
            src_ref=src, dst_ref=dst, send_sem=send, recv_sem=recv,
            device_id=to, device_id_type=MESH,
        )
        copy.start()
        sends.append(copy)

    def landed(slot, sem):
        pltpu.make_async_copy(slot, slot, sem).wait()

    def push_token(q, r, r_there, part, send, to):
        hk, cc = divmod(q, 2)
        push(token(hk, r, cc, part), token(hk, r_there, cc, part), send, tsem.at[hk, r_there, cc, part], to)

    def push_weight(zz, kind, i, send, to):
        push(weight(zz, kind, c, i), weight(zz, kind, c, i), send, wsem.at[zz, kind, c, i], to)

    barrier = pltpu.get_barrier_semaphore()
    peers = [{"z": zp}, {"z": zm}, {"x": xp}, {"x": xm}]
    peers += [
        {"l": (l + dl) % 2, "h": (h + dh) % 2, "c": (c + dc) % 2}
        for dl in (0, 1) for dh in (0, 1) for dc in (0, 1) if dl + dh + dc
    ]
    for peer in peers:
        pl.semaphore_signal(barrier, inc=1, device_id=peer, device_id_type=MESH)
    @pl.when(c == l)
    def _():
        for part in (0, 1):
            pltpu.make_async_copy(t_ref.at[half_rows(part)], token(0, 1, c, part), tsem.at[0, 1, c, part]).start()

    def stage(half, slot, row, k):
        src = w_ref.at[pl.ds(row * S, S), pl.ds(pl.multiple_of(half * S, S), S)]
        return pltpu.make_async_copy(src, slot, lsem.at[k, row])

    staged = [
        [stage(h, W.at[z, 0, (row - x + 5) % 4, c], row, 0) for row in range(4)],
        [stage(1 - h, G.at[(row - x + 5) % 4], row, 1) for row in range(4)],
    ]
    for copies in staged:
        for copy in copies:
            copy.start()
    pltpu.make_async_copy(b_ref, B.at[0], bsem.at[0]).start()

    for copy in staged[0]:
        copy.wait()
    pl.semaphore_wait(barrier, len(peers))

    def to_own_chip(part):
        return pltpu.make_async_remote_copy(
            src_ref=t_ref.at[half_rows(part)], dst_ref=token(0, 1, c, part),
            send_sem=ts_y.at[3, part], recv_sem=tsem.at[0, 1, c, part],
            device_id=sibling, device_id_type=MESH,
        )

    @pl.when(c != l)
    def _():
        to_own_chip(0).start()
        to_own_chip(1).start()

    def token_column(part, steps=(0, 1, 2)):
        for k in steps:
            yy = (yp, ym, (y + 2) % 4)[k]
            hk = (yy // 2 + h) % 2
            push(
                t_ref.at[half_rows(part)], token(hk, 1, c, part), ts_y.at[k, part], tsem.at[hk, 1, c, part],
                {"l": yy % 2, "h": yy // 2, "c": l},
            )

    def weight_column(i):
        push(G.at[:, :, pl.ds(i * C, C)], weight(z, 1, c, i), ws_a.at[i, 3], wsem.at[z, 1, c, i], {"h": 1 - h})

    for i in range(3):
        push_weight(z, 0, i, ws_a.at[i, 0], {"z": zp})
        push_weight(z, 0, i, ws_a.at[i, 1], {"z": zm})
    token_column(0)
    for copy in staged[1]:
        copy.wait()
    weight_column(0)
    token_column(1, (0, 1))
    weight_column(1)
    weight_column(2)
    token_column(1, (2,))
    for i in range(3):
        push_weight(z, 0, i, ws_a.at[i, 2], sibling)
    for k, (dh, dc) in enumerate(((0, 1), (1, 0), (1, 1))):
        to = {"h": (h + dh) % 2, "c": (c + dc) % 2}
        push(b_ref, B.at[1 + k], bs.at[k], bsem.at[1 + k], to)

    def token_in(q, r, part):
        hk, cc = divmod(q, 2)
        landed(token(hk, r, cc, part), tsem.at[hk, r, cc, part])

    def token_y(q, part):
        token_in(q, 1, part)
        push_token(q, 1, 0, part, ts_x.at[q, 0, part], {"x": xp})
        push_token(q, 1, 2, part, ts_x.at[q, 1, part], {"x": xm})

    def token_x(q, part):
        token_in(q, 0, part)
        if q % 2 == 0:
            push_token(q, 0, 3, part, ts_r.at[q, part], {"x": xp})
        token_in(q, 2, part)
        if q % 2 == 1:
            push_token(q, 2, 3, part, ts_r.at[q, part], {"x": xm})

    def weight_in(zz, kind, cc, i):
        landed(weight(zz, kind, cc, i), wsem.at[zz, kind, cc, i])

    def weight_y(i):
        weight_in(z, 1, c, i)
        push_weight(z, 1, i, ws_b.at[i, 0], {"z": zp})
        push_weight(z, 1, i, ws_b.at[i, 1], {"z": zm})
        push_weight(z, 1, i, ws_b.at[i, 2], sibling)

    def weight_z(kind, i):
        weight_in(zm, kind, c, i)
        push_weight(zm, kind, i, ws_n.at[0, kind, i], sibling)
        weight_in(zp, kind, c, i)
        push_weight(zp, kind, i, ws_n.at[1, kind, i], sibling)

    def relay(kind, i):
        near, to = ((zm, zp), (zp, zm))[kind]

        def part(r, count):
            return W.at[near, kind, pl.ds(r, count), c, :, pl.ds(i * C, C)]

        for k, slot in enumerate([part(0, 4)] if i < 2 else [part(0, 2), part(2, 2)]):
            push(slot, slot, ws_r.at[kind, i + k], wsem.at[near, kind, c, i + k], {"z": to})

    def weight_far(kind, i):
        weight_in(zf, kind, c, i)
        push_weight(zf, kind, i, ws_f.at[kind, i], sibling)

    def from_sibling(zz):
        for kind in (0, 1):
            for i in range(3):
                weight_in(zz, kind, other, i)

    def out_slot(ll, hh, rows=pl.ds(0, ROWS), first=0, width=S):
        return o_ref.at[rows, pl.ds(pl.multiple_of((2 * ll + hh) * S + first, C), width)]

    def out_remote(zz, k, rows, first, width):
        return pltpu.make_async_remote_copy(
            src_ref=O.at[k, rows, pl.ds(first, width)], dst_ref=out_slot(l, h, rows, first, width),
            send_sem=os.at[k, first // C], recv_sem=osem.at[2 * l + h],
            device_id={"l": c, "h": zz // 2, "c": zz % 2}, device_id_type=MESH,
        )

    def out_local(k, rows, first, width):
        return pltpu.make_async_copy(
            O.at[k, rows, pl.ds(first, width)], out_slot(l, h, rows, first, width), osem.at[2 * l + h]
        )

    def mine(zz):
        return jnp.logical_and(c == l, zz == g)

    def dot(rows, start, count, w):
        return jnp.dot(
            T[rows, pl.ds(start, count)], w.reshape(count, w.shape[-1]), preferred_element_type=jnp.float32
        )

    def finish(zz, k, rows, first, width, product):
        which = 2 * ((zz // 2 + h) % 2) + (zz % 2 + c) % 2
        parts = [
            B[which, pl.ds((2 * l + h) * 3 + t, 1), :] for t in range(first // C, (first + width) // C)
        ]
        bias = jnp.concatenate(parts, axis=1) if len(parts) > 1 else parts[0]
        pre = product + bias
        act = pre * (1.0 + lax.erf(pre * 0.7071067811865476)) * 0.5
        O[k, rows, pl.ds(first, width)] = act.astype(jnp.bfloat16)

        @pl.when(mine(zz))
        def _():
            out_local(k, rows, first, width).start()

        @pl.when(jnp.logical_not(mine(zz)))
        def _():
            out_remote(zz, k, rows, first, width).start()

    def columns(zz, k, part):
        finish(zz, k, half_rows(part), 0, S, dot(half_rows(part), 0, D, W[zz]))

    def far_columns(i, part):
        finish(zf, 3, half_rows(part), i * C, C, dot(half_rows(part), 0, D, W[zf, :, :, :, :, pl.ds(i * C, C)]))

    def last_columns(half, rows):
        w = [W[zf, kind, pl.ds(2 * half, 2), :, :, pl.ds(2 * C, C)] for kind in (0, 1)]
        product = sum(dot(rows, kind * HALF + half * 2 * PAIR, 2 * PAIR, w[kind]) for kind in (0, 1))
        if half == 0:
            A[rows, :] = product
        else:
            finish(zf, 3, rows, 2 * C, C, product + A[rows, :])

    for q in range(4):
        token_y(q, 0)
    weight_z(0, 0)
    token_x(0, 0)
    token_x(1, 0)
    weight_y(0)
    weight_z(0, 1)
    token_x(2, 0)
    token_x(3, 0)
    token_y(0, 1)
    token_y(1, 1)
    weight_z(0, 2)
    weight_y(1)
    weight_z(1, 0)
    token_x(0, 1)
    weight_y(2)
    for i in range(3):
        relay(0, i)
    relay(1, 0)
    token_x(1, 1)
    token_y(2, 1)
    token_y(3, 1)
    weight_z(1, 1)
    relay(1, 1)
    token_x(2, 1)
    token_x(3, 1)
    for k in range(4):
        landed(B.at[k], bsem.at[k])
    for q in range(4):
        token_in(q, 3, 0)
    from_sibling(z)
    columns(z, 0, 0)
    weight_z(1, 2)
    relay(1, 2)
    from_sibling(zm)
    columns(zm, 1, 0)
    from_sibling(zp)
    columns(zp, 2, 0)
    for q in range(4):
        token_in(q, 3, 1)
    columns(z, 0, 1)
    columns(zm, 1, 1)
    columns(zp, 2, 1)
    for i in range(4):
        for kind in (0, 1):
            weight_far(kind, i)
        for kind in (0, 1):
            weight_in(zf, kind, other, i)
        if i < 2:
            far_columns(i, 0)
            far_columns(i, 1)
        elif i == 2:
            for part in (0, 1):
                last_columns(0, half_rows(part))
        else:
            for first in range(0, ROWS, 128):
                last_columns(1, pl.ds(first, 128))

    for copy in sends:
        copy.wait_send()

    @pl.when(c != l)
    def _():
        to_own_chip(0).wait_send()
        to_own_chip(1).wait_send()

    for ll in (0, 1):
        for hh in (0, 1):
            landed(out_slot(ll, hh), osem.at[2 * ll + hh])


    all_rows = pl.ds(0, ROWS)
    whole = [(zz, k, all_rows, 0, S) for k, zz in enumerate((z, zm, zp))]
    for zz, *where in whole + [(zf, 3, all_rows, i * C, C) for i in range(3)]:
        @pl.when(jnp.logical_not(mine(zz)))
        def _():
            out_remote(zz, *where).wait_send()


def per_device(tokens, weight, bias):
    any_spec = pl.BlockSpec(memory_space=pl.ANY)
    dma = pltpu.SemaphoreType.DMA
    in_hbm = [pltpu.with_memory_space_constraint(a, pltpu.HBM) for a in (tokens, weight, bias.reshape(12, C))]
    return pl.pallas_call(
        kernel,
        out_shape=jax.ShapeDtypeStruct((ROWS, 4 * S), jnp.bfloat16),
        in_specs=[pl.BlockSpec(memory_space=pltpu.HBM)] * 3,
        out_specs=any_spec,
        scratch_shapes=[
            pltpu.VMEM((ROWS, D), jnp.bfloat16),
            pltpu.VMEM((4, 2, 4, 2, S, S), jnp.bfloat16),
            pltpu.VMEM((4, S, S), jnp.bfloat16),
            pltpu.VMEM((4, 12, C), jnp.float32),
            pltpu.VMEM((ROWS, C), jnp.float32),
            pltpu.VMEM((4, ROWS, S), jnp.bfloat16),
            dma((2, 4)), dma((2, 4, 2, 2)), dma((4, 2, 2, 4)), dma((4,)), dma((4,)),
            dma((4, 2)), dma((4, 2, 2)), dma((4, 2)), dma((3, 4)), dma((3, 3)),
            dma((2, 2, 3)), dma((2, 4)), dma((2, 4)), dma((3,)), dma((4, 3)),
        ],
        compiler_params=pltpu.CompilerParams(
            collective_id=0, has_side_effects=True, vmem_limit_bytes=48 * 2**20
        ),
    )(*in_hbm)


def solution(mesh):
    torus = Mesh(mesh.devices.reshape(4, 4, 2, 2, 2), ("x", "z", "l", "h", "c"))
    placed = (P(("z", "l"), ("h", "c", "x")), P(("h", "c"), ("x", "z", "l")), P(("x", "h", "c")))
    return jax.shard_map(
        per_device, mesh=torus, in_specs=placed, out_specs=P(("z", "l"), ("x", "h", "c")), check_vma=False
    )
```

```python
import jax
import jax.numpy as jnp
from jax import lax
from jax.experimental import pallas as pl
from jax.experimental.pallas import tpu as pltpu
from jax.sharding import Mesh
from jax.sharding import PartitionSpec as P

MESH = pl.DeviceIdType.MESH
S = 384
C = 128
ROWS = 512
D = 6144
TILE = 256

PAIR = 2 * S
HALF = 4 * PAIR


def kernel(
    t_ref, w_ref, b_ref, o_ref,
    T, W, G, B, A, O,
    lsem, tsem, wsem, bsem, osem,
    ts_y, ts_x, ts_r, ws_a, ws_b, ws_n, ws_r, ws_f, bs, os,
):
    x, z, l, h, c = (lax.axis_index(a) for a in ("x", "z", "l", "h", "c"))
    y = 2 * h + l
    g = 2 * h + c
    other = 1 - c
    xp, xm = (x + 1) % 4, (x + 3) % 4
    zp, zm, zf = (z + 1) % 4, (z + 3) % 4, (z + 2) % 4
    yp, ym = (y + 1) % 4, (y + 3) % 4
    sibling = {"c": other}
    sends = []

    def half_rows(part):
        return pl.ds(part * TILE, TILE)

    def token(hk, r, cc, part):
        return T.at[half_rows(part), pl.ds(pl.multiple_of(hk * HALF + r * PAIR + cc * S, S), S)]

    def weight(zz, hk, cc, i):
        if zz is zf and i >= 2:
            return W.at[zz, hk, pl.ds(2 * (i - 2), 2), cc, :, pl.ds(2 * C, C)]
        return W.at[zz, hk, :, cc, :, pl.ds(i * C, C)]

    def push(src, dst, send, recv, to):
        copy = pltpu.make_async_remote_copy(
            src_ref=src, dst_ref=dst, send_sem=send, recv_sem=recv,
            device_id=to, device_id_type=MESH,
        )
        copy.start()
        sends.append(copy)

    def landed(slot, sem):
        pltpu.make_async_copy(slot, slot, sem).wait()

    def push_token(q, r, r_there, part, send, to):
        hk, cc = divmod(q, 2)
        push(token(hk, r, cc, part), token(hk, r_there, cc, part), send, tsem.at[hk, r_there, cc, part], to)

    def push_weight(zz, kind, i, send, to):
        push(weight(zz, kind, c, i), weight(zz, kind, c, i), send, wsem.at[zz, kind, c, i], to)

    barrier = pltpu.get_barrier_semaphore()
    peers = [{"z": zp}, {"z": zm}, {"x": xp}, {"x": xm}]
    peers += [
        {"l": (l + dl) % 2, "h": (h + dh) % 2, "c": (c + dc) % 2}
        for dl in (0, 1) for dh in (0, 1) for dc in (0, 1) if dl + dh + dc
    ]
    for peer in peers:
        pl.semaphore_signal(barrier, inc=1, device_id=peer, device_id_type=MESH)
    @pl.when(c == l)
    def _():
        for part in (0, 1):
            pltpu.make_async_copy(t_ref.at[half_rows(part)], token(0, 1, c, part), tsem.at[0, 1, c, part]).start()

    def stage(half, slot, row, k):
        src = w_ref.at[pl.ds(row * S, S), pl.ds(pl.multiple_of(half * S, S), S)]
        return pltpu.make_async_copy(src, slot, lsem.at[k, row])

    staged = [
        [stage(h, W.at[z, 0, (row - x + 5) % 4, c], row, 0) for row in range(4)],
        [stage(1 - h, G.at[(row - x + 5) % 4], row, 1) for row in range(4)],
    ]
    for copies in staged:
        for copy in copies:
            copy.start()
    pltpu.make_async_copy(b_ref, B.at[0], bsem.at[0]).start()

    for copy in staged[0]:
        copy.wait()
    pl.semaphore_wait(barrier, len(peers))

    def to_own_chip(part):
        return pltpu.make_async_remote_copy(
            src_ref=t_ref.at[half_rows(part)], dst_ref=token(0, 1, c, part),
            send_sem=ts_y.at[3, part], recv_sem=tsem.at[0, 1, c, part],
            device_id=sibling, device_id_type=MESH,
        )

    @pl.when(c != l)
    def _():
        to_own_chip(0).start()
        to_own_chip(1).start()

    def token_column(part, steps=(0, 1, 2)):
        for k in steps:
            yy = (yp, ym, (y + 2) % 4)[k]
            hk = (yy // 2 + h) % 2
            push(
                t_ref.at[half_rows(part)], token(hk, 1, c, part), ts_y.at[k, part], tsem.at[hk, 1, c, part],
                {"l": yy % 2, "h": yy // 2, "c": l},
            )

    def weight_column(i):
        push(G.at[:, :, pl.ds(i * C, C)], weight(z, 1, c, i), ws_a.at[i, 3], wsem.at[z, 1, c, i], {"h": 1 - h})

    for i in range(3):
        push_weight(z, 0, i, ws_a.at[i, 0], {"z": zp})
        push_weight(z, 0, i, ws_a.at[i, 1], {"z": zm})
    token_column(0)
    for copy in staged[1]:
        copy.wait()
    weight_column(0)
    token_column(1, (0, 1))
    weight_column(1)
    weight_column(2)
    token_column(1, (2,))
    for i in range(3):
        push_weight(z, 0, i, ws_a.at[i, 2], sibling)
    for k, (dh, dc) in enumerate(((0, 1), (1, 0), (1, 1))):
        to = {"h": (h + dh) % 2, "c": (c + dc) % 2}
        push(b_ref, B.at[1 + k], bs.at[k], bsem.at[1 + k], to)

    def token_in(q, r, part):
        hk, cc = divmod(q, 2)
        landed(token(hk, r, cc, part), tsem.at[hk, r, cc, part])

    def token_y(q, part):
        token_in(q, 1, part)
        push_token(q, 1, 0, part, ts_x.at[q, 0, part], {"x": xp})
        push_token(q, 1, 2, part, ts_x.at[q, 1, part], {"x": xm})

    def token_x(q, part):
        token_in(q, 0, part)
        if q % 2 == 0:
            push_token(q, 0, 3, part, ts_r.at[q, part], {"x": xp})
        token_in(q, 2, part)
        if q % 2 == 1:
            push_token(q, 2, 3, part, ts_r.at[q, part], {"x": xm})

    def weight_in(zz, kind, cc, i):
        landed(weight(zz, kind, cc, i), wsem.at[zz, kind, cc, i])

    def weight_y(i):
        weight_in(z, 1, c, i)
        push_weight(z, 1, i, ws_b.at[i, 0], {"z": zp})
        push_weight(z, 1, i, ws_b.at[i, 1], {"z": zm})
        push_weight(z, 1, i, ws_b.at[i, 2], sibling)

    def weight_z(kind, i):
        weight_in(zm, kind, c, i)
        push_weight(zm, kind, i, ws_n.at[0, kind, i], sibling)
        weight_in(zp, kind, c, i)
        push_weight(zp, kind, i, ws_n.at[1, kind, i], sibling)

    def relay(kind, i):
        near, to = ((zm, zp), (zp, zm))[kind]

        def part(r, count):
            return W.at[near, kind, pl.ds(r, count), c, :, pl.ds(i * C, C)]

        for k, slot in enumerate([part(0, 4)] if i < 2 else [part(0, 2), part(2, 2)]):
            push(slot, slot, ws_r.at[kind, i + k], wsem.at[near, kind, c, i + k], {"z": to})

    def far_to_sibling(kind, i):
        slot = weight(zf, kind, c, i)
        return pltpu.make_async_remote_copy(
            src_ref=slot, dst_ref=slot, send_sem=ws_f.at[kind, i], recv_sem=wsem.at[zf, kind, c, i],
            device_id=sibling, device_id_type=MESH,
        )

    def weight_far(i):
        def in_turn(kinds):
            for kind in kinds:
                weight_in(zf, kind, c, i)
                far_to_sibling(kind, i).start()

        @pl.when(z == 0)
        def _():
            in_turn((1, 0))

        @pl.when(z != 0)
        def _():
            in_turn((0, 1))

    def from_sibling(zz):
        for kind in (0, 1):
            for i in range(3):
                weight_in(zz, kind, other, i)

    def out_slot(ll, hh, rows=pl.ds(0, ROWS), first=0, width=S):
        return o_ref.at[rows, pl.ds(pl.multiple_of((2 * ll + hh) * S + first, C), width)]

    def out_remote(zz, k, rows, first, width):
        return pltpu.make_async_remote_copy(
            src_ref=O.at[k, rows, pl.ds(first, width)], dst_ref=out_slot(l, h, rows, first, width),
            send_sem=os.at[k, first // C], recv_sem=osem.at[2 * l + h],
            device_id={"l": c, "h": zz // 2, "c": zz % 2}, device_id_type=MESH,
        )

    def out_local(k, rows, first, width):
        return pltpu.make_async_copy(
            O.at[k, rows, pl.ds(first, width)], out_slot(l, h, rows, first, width), osem.at[2 * l + h]
        )

    def mine(zz):
        return jnp.logical_and(c == l, zz == g)

    def dot(rows, start, count, w):
        return jnp.dot(
            T[rows, pl.ds(start, count)], w.reshape(count, w.shape[-1]), preferred_element_type=jnp.float32
        )

    def finish(zz, k, rows, first, width, product):
        which = 2 * ((zz // 2 + h) % 2) + (zz % 2 + c) % 2
        parts = [
            B[which, pl.ds((2 * l + h) * 3 + t, 1), :] for t in range(first // C, (first + width) // C)
        ]
        bias = jnp.concatenate(parts, axis=1) if len(parts) > 1 else parts[0]
        pre = product + bias
        act = pre * (1.0 + lax.erf(pre * 0.7071067811865476)) * 0.5
        O[k, rows, pl.ds(first, width)] = act.astype(jnp.bfloat16)

        @pl.when(mine(zz))
        def _():
            out_local(k, rows, first, width).start()

        @pl.when(jnp.logical_not(mine(zz)))
        def _():
            out_remote(zz, k, rows, first, width).start()

    def columns(zz, k, part):
        finish(zz, k, half_rows(part), 0, S, dot(half_rows(part), 0, D, W[zz]))

    def far_columns(i, part):
        finish(zf, 3, half_rows(part), i * C, C, dot(half_rows(part), 0, D, W[zf, :, :, :, :, pl.ds(i * C, C)]))

    def last_columns(half, rows):
        w = [W[zf, kind, pl.ds(2 * half, 2), :, :, pl.ds(2 * C, C)] for kind in (0, 1)]
        product = sum(dot(rows, kind * HALF + half * 2 * PAIR, 2 * PAIR, w[kind]) for kind in (0, 1))
        if half == 0:
            A[rows, :] = product
        else:
            finish(zf, 3, rows, 2 * C, C, product + A[rows, :])

    for q in range(4):
        token_y(q, 0)
    weight_z(0, 0)
    token_x(0, 0)
    token_x(1, 0)
    weight_y(0)
    weight_z(0, 1)
    token_x(2, 0)
    token_x(3, 0)
    token_y(0, 1)
    token_y(1, 1)
    weight_z(0, 2)
    weight_y(1)
    weight_z(1, 0)
    token_x(0, 1)
    weight_y(2)
    for i in range(3):
        relay(0, i)
    relay(1, 0)
    token_x(1, 1)
    token_y(2, 1)
    token_y(3, 1)
    weight_z(1, 1)
    relay(1, 1)
    token_x(2, 1)
    token_x(3, 1)
    for k in range(4):
        landed(B.at[k], bsem.at[k])
    for q in range(4):
        token_in(q, 3, 0)
    from_sibling(z)
    columns(z, 0, 0)
    weight_z(1, 2)
    relay(1, 2)
    from_sibling(zm)
    columns(zm, 1, 0)
    from_sibling(zp)
    columns(zp, 2, 0)
    for q in range(4):
        token_in(q, 3, 1)
    columns(z, 0, 1)
    columns(zm, 1, 1)
    columns(zp, 2, 1)
    for i in range(4):
        weight_far(i)
        for kind in (0, 1):
            weight_in(zf, kind, other, i)
        if i < 2:
            far_columns(i, 0)
            far_columns(i, 1)
        elif i == 2:
            for part in (0, 1):
                last_columns(0, half_rows(part))
        else:
            for first in range(0, ROWS, 128):
                last_columns(1, pl.ds(first, 128))

    for copy in sends:
        copy.wait_send()
    for i in range(4):
        for kind in (0, 1):
            far_to_sibling(kind, i).wait_send()

    @pl.when(c != l)
    def _():
        to_own_chip(0).wait_send()
        to_own_chip(1).wait_send()

    for ll in (0, 1):
        for hh in (0, 1):
            landed(out_slot(ll, hh), osem.at[2 * ll + hh])


    all_rows = pl.ds(0, ROWS)
    whole = [(zz, k, all_rows, 0, S) for k, zz in enumerate((z, zm, zp))]
    for zz, *where in whole + [(zf, 3, all_rows, i * C, C) for i in range(3)]:
        @pl.when(jnp.logical_not(mine(zz)))
        def _():
            out_remote(zz, *where).wait_send()


def per_device(tokens, weight, bias):
    any_spec = pl.BlockSpec(memory_space=pl.ANY)
    dma = pltpu.SemaphoreType.DMA
    in_hbm = [pltpu.with_memory_space_constraint(a, pltpu.HBM) for a in (tokens, weight, bias.reshape(12, C))]
    return pl.pallas_call(
        kernel,
        out_shape=jax.ShapeDtypeStruct((ROWS, 4 * S), jnp.bfloat16),
        in_specs=[pl.BlockSpec(memory_space=pltpu.HBM)] * 3,
        out_specs=any_spec,
        scratch_shapes=[
            pltpu.VMEM((ROWS, D), jnp.bfloat16),
            pltpu.VMEM((4, 2, 4, 2, S, S), jnp.bfloat16),
            pltpu.VMEM((4, S, S), jnp.bfloat16),
            pltpu.VMEM((4, 12, C), jnp.float32),
            pltpu.VMEM((ROWS, C), jnp.float32),
            pltpu.VMEM((4, ROWS, S), jnp.bfloat16),
            dma((2, 4)), dma((2, 4, 2, 2)), dma((4, 2, 2, 4)), dma((4,)), dma((4,)),
            dma((4, 2)), dma((4, 2, 2)), dma((4, 2)), dma((3, 4)), dma((3, 3)),
            dma((2, 2, 3)), dma((2, 4)), dma((2, 4)), dma((3,)), dma((4, 3)),
        ],
        compiler_params=pltpu.CompilerParams(
            collective_id=0, has_side_effects=True, vmem_limit_bytes=48 * 2**20
        ),
    )(*in_hbm)


def solution(mesh):
    torus = Mesh(mesh.devices.reshape(4, 4, 2, 2, 2), ("x", "z", "l", "h", "c"))
    placed = (P(("z", "l"), ("h", "c", "x")), P(("h", "c"), ("x", "z", "l")), P(("x", "h", "c")))
    return jax.shard_map(
        per_device, mesh=torus, in_specs=placed, out_specs=P(("z", "l"), ("x", "h", "c")), check_vma=False
    )
```
